128 devices in a mesh: freq: 32 (over x, z, core), tmpl: 4 (over y).
Axes of the slice: x: 4, y: 4, z: 4, core: 2. Of those that a mesh axis runs over, the one named last changes fastest.
Arguments:
- strain: bfloat16 [2, 16, 8388608], P(None, 'tmpl', 'freq'), may hold values from -6 to 6
- fiducial: bfloat16 [2, 16, 8388608], P(None, 'tmpl', 'freq'), may hold values from -6 to 6
- psd: float32 [16, 8388608], P('tmpl', 'freq'), may hold values from 0.25 to 8
- time_shift: float32 [16], P('tmpl'), may hold values from -8 to 8
- phase_shift: float32 [16], P('tmpl'), may hold values from -3.140625 to 3.140625
- bin_blocks: int32 [32, 128], replicated, may hold values from 1 to 32, as said below
- bin_owner: int32 [32, 128], replicated, may hold values from 0 to 31, as said below
Outputs:
- moved: bfloat16 [2, 16, 4096, 4096], P(None, 'tmpl', 'freq')
- summary: float32 [6, 16, 4096], P(None, 'tmpl', 'freq')
The draws below stay inside these ranges and needn't reach their ends.
Inputs may be any that keep to these rules, and one draw needn't show every extreme that they name: `bin_owner`: row p lists, in frequency order, the owners of the bins in the frequencies of index p of freq; each row names every owner exactly 4 times. `bin_blocks`: row p holds, in frequency order, the lengths in blocks of the bins in the frequencies of index p of freq; the 4 bins that row p hands to one owner total 2 * 32 blocks, and some bin of each row is 32 blocks long.
All inputs are finite; a program needn't handle non-finite values.
Results may differ from the reference program's by a relative error of at most 0.001.
The reference program's roundings to bfloat16 on the way (of `product`, `power` and `power_slots`) count: a program that leaves them out, or rounds other values in their place, can miss the bound.
Values may be sent and summed in bfloat16 or wider, within the bound.
No kernel may reach another device: no remote copies, remote signals or barrier semaphores. Data moves between devices by JAX's collectives and lax.ppermute only.
A program may use at most 128 MiB of HBM per device.

```python
import math
import jax
import jax.numpy as jnp

PAIR_BINS = 4
BINS_DEV = 128
BLK_DEV = 2048
MOST = 32
FREQS = 8388608
ROWS = 16
NBINS = 4096
N_FREQ = 32


def binning_tables(key):

    def one_row(position):
        row_key = jax.random.fold_in(key, position + 7)
        owners = (jax.random.permutation(jax.random.fold_in(row_key, 1), BINS_DEV) % N_FREQ).astype(jnp.int32)
        forced = jax.random.randint(jax.random.fold_in(row_key, 2), (), 0, N_FREQ)
        keys = jax.random.split(jax.random.fold_in(row_key, 3), 5)
        groups = jnp.arange(N_FREQ, dtype=jnp.int32)
        is_forced = groups == forced
        drawn_total = jax.random.randint(keys[0], (N_FREQ,), 2, 2 * MOST - 1)
        heavy_total = jax.random.randint(keys[1], (N_FREQ,), MOST + 1, 2 * MOST - 1)
        first_total = jnp.where(is_forced, heavy_total, drawn_total)
        first = jax.random.randint(keys[2], (N_FREQ,), jnp.maximum(1, first_total - MOST), jnp.minimum(MOST, first_total - 1) + 1)
        first = jnp.where(is_forced, MOST, first)
        second = first_total - first
        rest = 2 * MOST - first_total
        third = jax.random.randint(keys[3], (N_FREQ,), jnp.maximum(1, rest - MOST), jnp.minimum(MOST, rest - 1) + 1)
        fourth = rest - third
        stacked = jnp.stack([first, second, third, fourth], axis=1).astype(jnp.int32)
        order = jax.vmap(lambda sub: jax.random.permutation(sub, 4))(jax.random.split(keys[4], N_FREQ))
        stacked = jnp.take_along_axis(stacked, order.astype(jnp.int32), axis=1)
        position_ids = jnp.arange(BINS_DEV, dtype=jnp.int32)
        earlier = position_ids[None, :] < position_ids[:, None]
        same = owners[:, None] == owners[None, :]
        ranks = jnp.sum(jnp.logical_and(same, earlier).astype(jnp.int32), axis=1)
        lengths = stacked[owners, ranks]
        return (owners, lengths.astype(jnp.int32))
    return jax.vmap(one_row)(jnp.arange(N_FREQ, dtype=jnp.int32))


def draw_bin_owner(key, part):
    owners, lengths = binning_tables(jax.random.fold_in(key, 11))
    return owners.astype(jnp.int32)


def draw_bin_blocks(key, part):
    owners, lengths = binning_tables(jax.random.fold_in(key, 11))
    return lengths.astype(jnp.int32)


def shard_levels(own_key, dims, cuts, smallest, high):
    loudness, own = 1.0, jax.random.fold_in(own_key, 6)
    for dim, parts in cuts:
        draws = jnp.exp(jax.random.uniform(jax.random.fold_in(own, dim), (parts,), jnp.float32, smallest / len(cuts), high / len(cuts)))
        loudness = loudness * jnp.repeat(draws, dims[dim] // parts).reshape([-1 if axis == dim else 1 for axis in range(len(dims))])
    return loudness


def scatter_about(rng, dims, scale, bound, shards=(), kind=jnp.bfloat16):
    values = scale * jax.random.normal(rng, dims, jnp.float32)
    if shards:
        values = values * shard_levels(rng, dims, shards, -0.22, 0.18)
    return jnp.clip(values, -bound, bound).astype(kind)


def setup_inputs(seed: int = 0) -> dict:
    splits = jax.random.split(jax.random.key(seed), 8)
    return {
        "strain": scatter_about(splits[0], (2, ROWS, FREQS), 1.0, 6.0, ((1, 4), (2, 32))),
        "fiducial": scatter_about(splits[1], (2, ROWS, FREQS), 1.0, 6.0, ((1, 4), (2, 32))),
        "psd": jnp.clip(jnp.exp(math.log(8.0) - 3.465736 * jax.random.uniform(splits[2], (ROWS, FREQS), jnp.float32) ** shard_levels(splits[2], (ROWS, FREQS), ((0, 4), (1, 32)), -0.2, 0.2)), 0.25, 8.0),
        "time_shift": jnp.clip(jax.random.uniform(splits[3], (ROWS,), jnp.float32, -8.0, 8.0) * shard_levels(splits[3], (ROWS,), ((0, 4),), -0.4, 0.0), -8.0, 8.0),
        "phase_shift": jnp.clip(jax.random.uniform(splits[4], (ROWS,), jnp.float32, -3.140625, 3.140625), -3.140625, 3.140625),
        "bin_blocks": draw_bin_blocks(jax.random.fold_in(splits[7], 71), 0),
        "bin_owner": draw_bin_owner(jax.random.fold_in(splits[7], 71), 0),
    }


two_pi = 2.0 * math.pi
ratio_scale = 1.0 / 64.0
power_scale = 1.0 / 2048.0


def heterodyne(strain, fiducial, weight, time_shift, phase_shift, unit):
    strain_re = strain[0].astype(jnp.float32)
    strain_im = strain[1].astype(jnp.float32)
    fid_re = fiducial[0].astype(jnp.float32)
    fid_im = fiducial[1].astype(jnp.float32)
    angle = (two_pi * time_shift)[:, None] * unit[None, :] + phase_shift[:, None]
    cosine = jnp.cos(angle)
    sine_val = jnp.sin(angle)
    cross_re = strain_re * fid_re + strain_im * fid_im
    cross_im = strain_im * fid_re - strain_re * fid_im
    prod_re = weight * (cross_re * cosine + cross_im * sine_val)
    prod_im = weight * (cross_im * cosine - cross_re * sine_val)
    product = jnp.stack([prod_re, prod_im]).astype(jnp.bfloat16)
    power = (weight * (fid_re * fid_re + fid_im * fid_im)).astype(jnp.bfloat16)
    return product, power


def slot_tables(bin_blocks, bin_owner):
    count = bin_blocks.shape[1]
    starts = jnp.cumsum(bin_blocks, axis=1).astype(jnp.int32) - bin_blocks
    position = jnp.arange(count, dtype=jnp.int32)
    earlier = position[None, :] < position[:, None]
    same = bin_owner[:, :, None] == bin_owner[:, None, :]
    ranks = jnp.sum(jnp.logical_and(same, earlier[None]).astype(jnp.int32), axis=2)
    return starts, ranks


def arrange(values, first_block, lengths, most_blocks):
    lead = values.shape[:-1]
    blocks = values.shape[-1] // 128
    tiled = values.reshape(lead + (blocks, 128))
    step_ids = jnp.arange(most_blocks, dtype=jnp.int32)
    block_ids = jnp.minimum(first_block[:, None] + step_ids[None, :], blocks - 1)
    picked = jnp.take(tiled, block_ids.reshape(-1), axis=values.ndim - 1)
    slot_count = first_block.shape[0]
    picked = picked.reshape(lead + (slot_count, most_blocks, 128))
    live = (step_ids[None, :] < lengths[:, None])[:, :, None]
    picked = jnp.where(live, picked, jnp.zeros((), values.dtype))
    return picked.reshape(lead + (slot_count, most_blocks * 128))


def summarize(moved, power_slots, lengths):
    width = moved.shape[-1]
    offset = (jnp.arange(width, dtype=jnp.int32).astype(jnp.float32)[None, :] + 0.5
              - 64.0 * lengths.astype(jnp.float32)[:, None]) / 128.0
    values = moved.astype(jnp.float32)
    weighted = power_slots[0].astype(jnp.float32)
    plain_sum = jnp.sum(values, axis=-1) * ratio_scale
    slope_sum = jnp.sum(values * offset, axis=-1) * ratio_scale
    power_sum = jnp.sum(weighted, axis=-1) * power_scale
    power_slope = jnp.sum(weighted * offset, axis=-1) * power_scale
    return jnp.concatenate([plain_sum, slope_sum, power_sum[None], power_slope[None]], axis=0)


def reference(strain, fiducial, psd, time_shift, phase_shift, bin_blocks, bin_owner):
    padded = jnp.pad(psd, ((0, 0), (1, 1)))
    weight = 1.0 / (0.25 * (padded[:, :-2] + 2.0 * padded[:, 1:-1] + padded[:, 2:]))
    unit = jnp.arange(FREQS, dtype=jnp.int32).astype(jnp.float32) / FREQS
    product, power = heterodyne(strain, fiducial, weight, time_shift, phase_shift, unit)
    starts, ranks = slot_tables(bin_blocks, bin_owner)
    source = jnp.arange(N_FREQ, dtype=jnp.int32)[:, None]
    slots = (bin_owner * BINS_DEV + source * PAIR_BINS + ranks).reshape(-1)
    first_block = jnp.zeros((NBINS,), jnp.int32).at[slots].set((source * BLK_DEV + starts).reshape(-1))
    lengths = jnp.zeros((NBINS,), jnp.int32).at[slots].set(bin_blocks.reshape(-1))
    moved = arrange(product, first_block, lengths, MOST)
    power_slots = arrange(power, first_block, lengths, MOST)[None]
    summary = summarize(moved, power_slots, lengths)
    return moved, summary
```

```python
import functools
import math

import jax
import jax.numpy as jnp
from jax import lax
from jax.experimental import pallas as pl
from jax.experimental.pallas import tpu as pltpu
from jax.sharding import PartitionSpec as P

TWO_PI = 2.0 * math.pi
RATIO_SCALE = 1.0 / 64.0
POWER_SCALE = 1.0 / 2048.0
LANES = 128
SUB = 8
ROWS = 4
STEPS = 32
BF = jnp.bfloat16
F32 = jnp.float32


def pack_kernel(chunks, blocks_ref, owner_ref, ts_ref, ps_ref, left_ref, right_ref, psd_hbm, strain_hbm, fid_hbm,
                out_ref, psd_s, strain_s, fid_s, pw_s, trig_v, trig_u, where_s, bin_s, pos_ref, start_ref, slot_ref,
                total_s, count_s, sem_p, sem_s, sem_f, sem_t):
    me = lax.axis_index("freq")
    n_freq = lax.axis_size("freq")
    rows = psd_hbm.shape[0]
    blocks = rows // ROWS
    bins = blocks_ref.shape[1]
    part = rows // chunks
    pair = blocks // n_freq + 1

    def copies(i):
        at = pl.ds(pl.multiple_of(i * part, part), part)
        return (
            pltpu.make_async_copy(psd_hbm.at[at], psd_s.at[pl.ds(pl.multiple_of(SUB + i * part, SUB), part)], sem_p.at[i]),
            pltpu.make_async_copy(strain_hbm.at[:, at], strain_s.at[:, at], sem_s.at[i]),
            pltpu.make_async_copy(fid_hbm.at[:, at], fid_s.at[:, at], sem_f.at[i]),
        )

    for i in range(chunks):
        for c in copies(i):
            c.start()

    def clear(d, carry):
        total_s[d] = 0
        count_s[d] = 0
        return carry

    lax.fori_loop(0, n_freq, clear, 0, unroll=8)
    shape = where_s.shape
    block = lax.broadcasted_iota(jnp.int32, shape, 0) * LANES + lax.broadcasted_iota(jnp.int32, shape, 1)

    def step(j, carry):
        start, previous, acc = carry
        owner = owner_ref[me, j]
        length = blocks_ref[me, j]
        used = total_s[owner]
        rank = count_s[owner]
        total_s[owner] = used + length
        count_s[owner] = rank + 1
        base = owner * pair + used - start
        start_ref[j] = start
        slot_ref[j] = owner * 4 + rank
        acc = acc + jnp.where(block >= start, base - previous, 0)
        return start + length, base, acc

    _, _, acc = lax.fori_loop(0, bins, step, (jnp.int32(0), jnp.int32(0), block), unroll=4)
    where_s[...] = acc
    to_smem = pltpu.make_async_copy(where_s, pos_ref, sem_t)
    to_smem.start()

    row = lax.broadcasted_iota(jnp.int32, (SUB, LANES), 0)
    lane = lax.broadcasted_iota(jnp.int32, (SUB, LANES), 1)
    r = row % ROWS
    upper = row // ROWS

    def spread(ref):
        return jnp.where(r == 0, ref[0], jnp.where(r == 1, ref[1], jnp.where(r == 2, ref[2], ref[3])))

    total = LANES * blocks * n_freq
    rate = TWO_PI * spread(ts_ref)
    phase = spread(ps_ref)
    psd_s[ROWS:SUB] = left_ref[...]
    psd_s[SUB + rows:SUB + rows + ROWS] = right_ref[...]

    pairs = blocks // 2
    outer = pairs // STEPS

    def trig(v, carry):
        at = pl.ds(pl.multiple_of(v * SUB, SUB), SUB)
        inside = ((2 * v + upper) * LANES + lane).astype(F32) / total
        angle = rate * inside
        trig_v[0, at] = jnp.cos(angle)
        trig_v[1, at] = jnp.sin(angle)
        first = (me * (blocks * LANES) + v * (2 * STEPS * LANES)).astype(F32) / total
        angle = rate * first + phase
        trig_u[0, at] = jnp.cos(angle)
        trig_u[1, at] = jnp.sin(angle)
        return carry

    assert outer == STEPS
    lax.fori_loop(0, STEPS, trig, 0)
    to_smem.wait()

    first_lane = lane == 0
    last_lane = lane == LANES - 1
    group = 8

    def body(base, spots, cu, su, v0):
        base = pl.multiple_of(base, SUB * group)
        slab = pl.ds(base, SUB * group)
        mids = psd_s[pl.ds(base + SUB, SUB * group)]
        lows = psd_s[pl.ds(base + SUB - ROWS, SUB * group)]
        highs = psd_s[pl.ds(base + SUB + ROWS, SUB * group)]
        s_res, s_ims = strain_s[0, slab], strain_s[1, slab]
        f_res, f_ims = fid_s[0, slab], fid_s[1, slab]
        vat = pl.ds(pl.multiple_of(v0, SUB * group), SUB * group)
        cvs, svs = trig_v[0, vat], trig_v[1, vat]
        powers = []
        for q in range(group):
            at = slice(q * SUB, (q + 1) * SUB)
            mid = mids[at]
            before = pltpu.roll(jnp.where(last_lane, lows[at], mid), 1, 1)
            after = pltpu.roll(jnp.where(first_lane, highs[at], mid), LANES - 1, 1)
            weight = 1.0 / (0.25 * (before + 2.0 * mid + after))
            s_re, s_im = s_res[at].astype(F32), s_ims[at].astype(F32)
            f_re, f_im = f_res[at].astype(F32), f_ims[at].astype(F32)
            cv, sv = cvs[at], svs[at]
            cosine = cu * cv - su * sv
            sine = su * cv + cu * sv
            cross_re = s_re * f_re + s_im * f_im
            cross_im = s_im * f_re - s_re * f_im
            re = weight * (cross_re * cosine + cross_im * sine)
            im = weight * (cross_im * cosine - cross_re * sine)
            power = weight * (f_re * f_re + f_im * f_im)
            powers.append(power.astype(BF).astype(F32))
            re_swap = pltpu.roll(re, ROWS, 0)
            im_swap = pltpu.roll(im, ROWS, 0)
            out_ref[spots[2 * q]] = jnp.where(upper == 0, re, im_swap).astype(BF)
            out_ref[spots[2 * q + 1]] = jnp.where(upper == 0, re_swap, im).astype(BF)
        pw_s[slab] = jnp.concatenate(powers, axis=0)

    per = outer // chunks
    turns = STEPS // group
    copies(0)[0].wait()

    def chunk_body(k, carry):
        @pl.when(k + 1 < chunks)
        def _():
            copies(k + 1)[0].wait()

        c = copies(k)
        c[1].wait()
        c[2].wait()
        for w in range(per):
            u = k * per + w
            uat = pl.ds(pl.multiple_of(u * SUB, SUB), SUB)
            cu = trig_u[0, uat]
            su = trig_u[1, uat]

            def inner(t, c, u=u, cu=cu, su=su):
                first = u * STEPS + t * group
                pos_row = lax.shift_right_logical(first, 6)
                pos_col = lax.bitwise_and(first, 63) * 2
                spots = [pos_ref[pos_row, pos_col + q] for q in range(2 * group)]
                body(first * SUB, spots, cu, su, t * group * SUB)
                return c

            lax.fori_loop(0, turns, inner, 0)
        return carry

    lax.fori_loop(0, chunks, chunk_body, 0)

    lane_off = (lane.astype(F32) + (0.5 - 64.0)) / 128.0

    def bin_body(j, carry):
        start = start_ref[j]
        length = blocks_ref[me, j]
        acc0 = jnp.zeros((SUB, LANES), F32)
        acc1 = jnp.zeros((SUB, LANES), F32)
        for t in range(STEPS // 2):
            x = jnp.where(upper < length - 2 * t, pw_s[pl.ds(start * ROWS + t * SUB, SUB)], 0.0)
            acc0 = acc0 + x
            acc1 = acc1 + acc0
        middle = float(STEPS) - (length - 1).astype(F32) * 0.5
        acc1 = acc0 * (lane_off + upper.astype(F32) + middle) - 2.0 * acc1
        acc0 = acc0 + pltpu.roll(acc0, ROWS, 0)
        acc1 = acc1 + pltpu.roll(acc1, ROWS, 0)
        bin_s[slot_ref[j]] = jnp.where(upper == 0, acc0, acc1)
        return carry

    lax.fori_loop(0, bins, bin_body, 0, unroll=2)

    def owner_body(d, carry):
        tile = jnp.zeros((SUB, LANES), F32)
        for k in range(4):
            sums = jnp.sum(bin_s[d * 4 + k], axis=1, keepdims=True)
            high = sums.astype(BF).astype(F32)
            rest = sums - high
            mid = rest.astype(BF).astype(F32)
            tile = jnp.where(lane == 3 * k, high, tile)
            tile = jnp.where(lane == 3 * k + 1, mid, tile)
            tile = jnp.where(lane == 3 * k + 2, rest - mid, tile)
        out_ref[d * pair + pair - 1] = tile.astype(BF)
        return carry

    lax.fori_loop(0, n_freq, owner_body, 0, unroll=4)


def unpack_kernel(groups, pair, lens_ref, got_hbm, moved_ref, sum_ref, got_s, turn, sems):
    g = pl.program_id(0)
    steps = sems.shape[0]
    part = 2 * groups * pair
    lane = lax.broadcasted_iota(jnp.int32, (SUB, LANES), 1)
    unroll = turn.shape[0]

    def fetch(i):
        at = pl.ds(i * part, part)
        return pltpu.make_async_copy(got_hbm.at[at], got_s.at[at], sems.at[i])

    @pl.when(g == 0)
    def _():
        for i in range(steps):
            fetch(i).start()
        sum_ref[...] = jnp.zeros_like(sum_ref)

    fetch(g).wait()

    def one(h, nothing):
        first = g * groups + h
        lens, bases, limits = [], [], []
        for i in range(SUB):
            p, k = 2 * first + i // 4, i % 4
            base = p * pair
            for q in range(k):
                base = base + lens_ref[p, q]
            lens.append(lens_ref[p, k])
            bases.append(base)
            limits.append(jnp.full((SUB, LANES), lens[i], jnp.int32))

        def cols(t, carry):
            acc0, acc1 = list(carry[0]), list(carry[1])
            xs = [got_ref_slab(bases[i] + t * unroll) for i in range(SUB)]
            for w in range(unroll):
                j = t * unroll + w
                here = jnp.full((SUB, LANES), j, jnp.int32)
                buf = turn.at[w]
                for i in range(SUB):
                    x = jnp.where(here < limits[i], xs[i][w].astype(F32), 0.0)
                    acc0[i] = acc0[i] + x
                    acc1[i] = acc1[i] + acc0[i]
                    buf[pl.ds(9 * i, SUB)] = x
                at = pl.ds(pl.multiple_of(j * LANES, LANES), LANES)
                to = pl.ds(pl.multiple_of(h * SUB, SUB), SUB)
                for q in range(SUB):
                    moved_ref[q // ROWS, q % ROWS, to, at] = buf[pl.ds(q, SUB, stride=9)].astype(BF)
            return tuple(acc0), tuple(acc1)

        def got_ref_slab(at):
            return got_s[pl.ds(at, unroll)]

        zero = tuple(jnp.zeros((SUB, LANES), F32) for _ in range(SUB))
        acc0, acc1 = lax.fori_loop(0, STEPS // unroll, cols, (zero, zero))

        plain, slope, power = sum_ref[0:8], sum_ref[8:16], sum_ref[16:24]
        for i in range(SUB):
            here = lane == first * SUB + i
            off = (lane.astype(F32) + 0.5 - 64.0 * lens[i].astype(F32)) / 128.0 + float(STEPS)
            tilt = acc0[i] * off - acc1[i]
            plain = jnp.where(here, jnp.sum(acc0[i], axis=1, keepdims=True) * RATIO_SCALE, plain)
            slope = jnp.where(here, jnp.sum(tilt, axis=1, keepdims=True) * RATIO_SCALE, slope)
            x = got_s[(2 * first + i // 4) * pair + pair - 1].astype(F32)
            x = jnp.where(jnp.logical_and(lane >= 3 * (i % 4), lane < 3 * (i % 4) + 3), x, 0.0)
            power = jnp.where(here, jnp.sum(x, axis=1, keepdims=True) * POWER_SCALE, power)
        sum_ref[0:8] = plain
        sum_ref[8:16] = slope
        sum_ref[16:24] = power
        return nothing

    lax.fori_loop(0, groups, one, 0)


def shift(array, up):
    n = lax.axis_size("freq")
    links = [(i, i + 1) if up else (i + 1, i) for i in range(n - 1)]
    return lax.ppermute(array, "freq", links)


def local(strain, fiducial, psd, time_shift, phase_shift, bin_blocks, bin_owner):
    n_freq = lax.axis_size("freq")
    me = lax.axis_index("freq")
    width = psd.shape[1]
    blocks = width // LANES
    bins = bin_blocks.shape[1]
    pair = blocks // n_freq + 1
    rows = blocks * ROWS
    chunks = 16
    smem = pl.BlockSpec(memory_space=pltpu.SMEM)
    vmem = pl.BlockSpec(memory_space=pltpu.VMEM)
    hbm = pl.BlockSpec(memory_space=pl.ANY)

    left = shift(psd[:, width - LANES:], True)
    right = shift(psd[:, :LANES], False)

    def tile(array):
        lead = array.shape[:-2]
        split = array.reshape(lead + (ROWS, blocks, LANES))
        return jnp.swapaxes(split, -3, -2).reshape(lead + (rows, LANES))

    packed = pl.pallas_call(
        functools.partial(pack_kernel, chunks),
        out_shape=jax.ShapeDtypeStruct((n_freq * pair, SUB, LANES), BF),
        in_specs=[smem] * 4 + [vmem] * 2 + [hbm] * 3,
        out_specs=vmem,
        scratch_shapes=[
            pltpu.VMEM((rows + 2 * SUB, LANES), F32),
            pltpu.VMEM((2, rows, LANES), BF),
            pltpu.VMEM((2, rows, LANES), BF),
            pltpu.VMEM((rows + STEPS * ROWS, LANES), F32),
            pltpu.VMEM((2, STEPS * SUB, LANES), F32),
            pltpu.VMEM((2, STEPS * SUB, LANES), F32),
            pltpu.VMEM((blocks // LANES, LANES), jnp.int32),
            pltpu.VMEM((bins, SUB, LANES), F32),
            pltpu.SMEM((blocks // LANES, LANES), jnp.int32),
            pltpu.SMEM((bins,), jnp.int32),
            pltpu.SMEM((bins,), jnp.int32),
            pltpu.SMEM((n_freq,), jnp.int32),
            pltpu.SMEM((n_freq,), jnp.int32),
            pltpu.SemaphoreType.DMA((chunks,)),
            pltpu.SemaphoreType.DMA((chunks,)),
            pltpu.SemaphoreType.DMA((chunks,)),
            pltpu.SemaphoreType.DMA,
        ],
        compiler_params=pltpu.CompilerParams(vmem_limit_bytes=60 * 1024 * 1024),
        name="pack",
    )(bin_blocks, bin_owner, time_shift, phase_shift, left, right, tile(psd), tile(strain), tile(fiducial))

    got = lax.all_to_all(
        packed.reshape(n_freq, pair, SUB, LANES), "freq", split_axis=0, concat_axis=0, tiled=True
    ).reshape(n_freq * pair, SUB, LANES)

    mine = (bin_owner == me).astype(jnp.int32)
    rank = jnp.cumsum(mine, axis=1) - 1
    key = jnp.where(mine == 1, rank, -1)
    lens = jnp.sum(
        jnp.where(key[:, None, :] == jnp.arange(4, dtype=jnp.int32)[None, :, None], bin_blocks[:, None, :], 0), axis=2
    )

    groups = 2
    moved, summary = pl.pallas_call(
        functools.partial(unpack_kernel, groups, pair),
        grid=(n_freq // 2 // groups,),
        out_shape=(
            jax.ShapeDtypeStruct((2, ROWS, bins, STEPS * LANES), BF),
            jax.ShapeDtypeStruct((6 * ROWS, bins), F32),
        ),
        in_specs=[
            smem,
            hbm,
        ],
        out_specs=(
            pl.BlockSpec((2, ROWS, SUB * groups, STEPS * LANES), lambda g: (0, 0, g, 0)),
            pl.BlockSpec((6 * ROWS, bins), lambda g: (0, 0)),
        ),
        scratch_shapes=[
            pltpu.VMEM((n_freq * pair + STEPS, SUB, LANES), BF),
            pltpu.VMEM((4, 9 * SUB, LANES), F32),
            pltpu.SemaphoreType.DMA((n_freq // 2 // groups,)),
        ],
        compiler_params=pltpu.CompilerParams(vmem_limit_bytes=60 * 1024 * 1024),
        name="unpack",
    )(lens, got)
    return moved, summary.reshape(6, ROWS, bins)


def solution(mesh):
    return jax.shard_map(
        local,
        mesh=mesh,
        in_specs=(
            P(None, "tmpl", "freq"),
            P(None, "tmpl", "freq"),
            P("tmpl", "freq"),
            P("tmpl"),
            P("tmpl"),
            P(),
            P(),
        ),
        out_specs=(P(None, "tmpl", "freq", None), P(None, "tmpl", "freq")),
        check_vma=False,
    )
```
